32 devices in a mesh: group: 8 (over z, y), tok: 4 (over x, core).
Axes of the slice: x: 2, y: 2, z: 4, core: 2. Of those that a mesh axis runs over, the one named last changes fastest.
Arguments:
- tokens: bfloat16 [16384, 2048], P(('group', 'tok')), may hold values from -94 to 94
- learning_rates: float32 [2, 16384], P(None, 'group'), may hold values from 0.1 to 1
- channel_gains: float32 [2, 5, 2048], P(None, None, 'tok'), may hold values from 0.3 to 3
- fast_init: float32 [2, 3, 16, 128, 128], P(None, None, 'tok'), may hold values from -0.5 to 0.5
- step_size: float32 [2, 16], P(None, 'tok'), may hold values from 0.05 to 1
- update_table: int32 [2, 8], replicated, may hold values 0 or 1
Outputs:
- mixed: bfloat16 [16384, 2048], P(('group', 'tok'))
The draws below stay inside these ranges and needn't reach their ends.
All inputs are finite; a program needn't handle non-finite values.
Results may differ from the reference program's by a relative error of at most 0.033.
Values may be sent and summed in bfloat16 or wider, within the bound.
A program may use at most 64 MiB of HBM per device.

```python
import math
import jax
import jax.numpy as jnp
from jax import lax

D = 2048
HEADS = 16
HEAD = 128
LAYERS = 2
NS_STEPS = 5
GROUPS = 8
GROUP_TOK = 2048
TOKENS = 16384


def draw_tokens(key, part):
    key_base = jax.random.fold_in(key, 11)
    key_jitter = jax.random.fold_in(key, 12)
    normal_draw = jnp.clip(jax.random.normal(key_base, (TOKENS, D), jnp.float32), -6.0, 6.0)
    channel_ramp = 3.0 ** (jnp.arange(D, dtype=jnp.float32) / D)
    jitter = jax.random.uniform(key_jitter, (D,), jnp.float32, 0.7, 1.3)
    values = normal_draw * (channel_ramp * jitter)[None, :]
    return values.astype(jnp.bfloat16)


def plant(array, own_key, least, largest):
    extent = array.shape
    index_at = [jax.random.randint(jax.random.fold_in(own_key, axis), (), 0, extent[axis]) for axis in range(len(extent))]
    array = array.at[tuple(index_at)].set(least)
    longest = extent.index(max(extent))
    index_at[longest] = (index_at[longest] + 1) % extent[longest]
    return array.at[tuple(index_at)].set(largest)


def steps_of(rng, dims, cuts, least, largest):
    def one(dim, shards_of):
        heights = jax.random.uniform(jax.random.fold_in(jax.random.fold_in(rng, 6), dim), (shards_of,), jnp.float32, least / len(cuts), largest / len(cuts))
        return jnp.repeat(jnp.exp(heights), dims[dim] // shards_of).reshape((-1,) + (1,) * (len(dims) - dim - 1))

    loudness = one(*cuts[0])
    for cut in cuts[1:]:
        loudness = loudness * one(*cut)
    return loudness


def normal_values(own_key, shape, deviation, most, pieces=(), held_as=jnp.bfloat16):
    level = steps_of(own_key, shape, pieces, -0.22, 0.18) if pieces else 1.0
    result = jax.random.normal(own_key, shape, jnp.float32) * deviation * level
    return jnp.minimum(jnp.maximum(result, -most), most).astype(held_as)


def setup_inputs(seed: int = 0) -> dict:
    splits = jax.random.split(jax.random.key(seed), 7)
    return {
        "tokens": draw_tokens(jax.random.fold_in(splits[6], 71), 0),
        "learning_rates": jnp.clip(jnp.exp(math.log(1.0) - 2.3025851 * jax.random.uniform(splits[1], (LAYERS, TOKENS), jnp.float32) ** steps_of(splits[1], (LAYERS, TOKENS), ((1, 8),), -0.2, 0.2)), 0.1, 1.0),
        "channel_gains": jnp.clip(jnp.exp(math.log(3.0) - 2.3025851 * jax.random.uniform(splits[2], (LAYERS, 5, D), jnp.float32) ** steps_of(splits[2], (LAYERS, 5, D), ((2, 4),), -0.2, 0.2)), 0.3, 3.0),
        "fast_init": normal_values(splits[3], (LAYERS, 3, HEADS, HEAD, HEAD), HEAD ** -0.5, 0.5, ((2, 4),), jnp.float32),
        "step_size": jnp.clip(jnp.exp(math.log(1.0) - 2.9957323 * jax.random.uniform(splits[4], (LAYERS, HEADS), jnp.float32) ** steps_of(splits[4], (LAYERS, HEADS), ((1, 4),), -0.2, 0.2)), 0.05, 1.0),
        "update_table": plant((jax.random.randint(splits[5], (LAYERS, GROUPS), 0, 4) < 3).astype(jnp.int32), jax.random.fold_in(splits[5], 1), 0, 1),
    }


MUON_A = 3.4445
MUON_B = -4.775
MUON_C = 2.0315
EPSILON = 1e-06

def orthogonalize(gradient):
    scaling = lax.rsqrt(lax.optimization_barrier(jnp.sum(gradient * gradient, axis=(-2, -1), keepdims=True)) + EPSILON)
    current = gradient * scaling
    for repeat in range(NS_STEPS):
        square = jnp.einsum('...ij,...kj->...ik', current, current, precision=lax.Precision.HIGHEST)
        polynom = MUON_B * square + MUON_C * jnp.einsum('...ij,...jk->...ik', square, square, precision=lax.Precision.HIGHEST)
        current = MUON_A * current + jnp.einsum('...ij,...jk->...ik', polynom, current, precision=lax.Precision.HIGHEST)
    return current

def layer_group(stream, entering, gain_rows, rates_row, steps_row, update_flag, inverse):
    row_count, channel_count = stream.shape
    heads_n = entering.shape[1]
    head_dim = entering.shape[2]
    normed = stream.astype(jnp.float32) * inverse[:, None] * gain_rows[0]
    queries = (normed * gain_rows[1]).astype(jnp.bfloat16).reshape(row_count, heads_n, head_dim).astype(jnp.float32)
    keys_in = (normed * gain_rows[2]).astype(jnp.bfloat16).reshape(row_count, heads_n, head_dim).astype(jnp.float32)
    values_in = (normed * gain_rows[3]).astype(jnp.bfloat16).reshape(row_count, heads_n, head_dim).astype(jnp.float32)
    rounded = entering.astype(jnp.bfloat16).astype(jnp.float32)
    gate_q = jnp.einsum('thi,hij->thj', queries, rounded[0])
    up_q = jnp.einsum('thi,hij->thj', queries, rounded[1])
    hidden_q = (jax.nn.silu(gate_q) * up_q).astype(jnp.bfloat16).astype(jnp.float32)
    output = jnp.einsum('thj,hjk->thk', hidden_q, rounded[2]).reshape(row_count, channel_count)
    mixed_rows = (stream.astype(jnp.float32) + gain_rows[4] * output).astype(jnp.bfloat16)
    gate_k = jnp.einsum('thi,hij->thj', keys_in, rounded[0])
    up_k = jnp.einsum('thi,hij->thj', keys_in, rounded[1])
    sigmoid_k = jax.nn.sigmoid(gate_k)
    active_k = gate_k * sigmoid_k
    hidden_k = (active_k * up_k).astype(jnp.bfloat16).astype(jnp.float32)
    targets = (rates_row[:, None, None] * values_in).astype(jnp.bfloat16).astype(jnp.float32)
    back_hidden = jnp.einsum('thk,hjk->thj', targets, rounded[2])
    back_up = (back_hidden * active_k).astype(jnp.bfloat16).astype(jnp.float32)
    back_gate = (back_hidden * up_k * sigmoid_k * (1.0 + gate_k * (1.0 - sigmoid_k))).astype(jnp.bfloat16).astype(jnp.float32)
    grad_gate = jnp.einsum('thi,thj->hij', keys_in, back_gate)
    grad_up = jnp.einsum('thi,thj->hij', keys_in, back_up)
    grad_down = jnp.einsum('thj,thk->hjk', hidden_k, targets)
    direction = orthogonalize(jnp.stack([grad_gate, grad_up, grad_down]))
    moved_state = entering + (update_flag * steps_row)[None, :, None, None] * direction
    norm_before = jnp.sqrt(lax.optimization_barrier(jnp.sum(entering * entering, axis=2, keepdims=True)) + EPSILON)
    norm_after = jnp.sqrt(lax.optimization_barrier(jnp.sum(moved_state * moved_state, axis=2, keepdims=True)) + EPSILON)
    return (mixed_rows, moved_state * (norm_before / norm_after))

def reference(tokens, learning_rates, channel_gains, fast_init, step_size, update_table):
    stream = tokens.reshape(GROUPS, GROUP_TOK, D)
    for layer_index in range(LAYERS):

        def advance(weights, inputs):
            block_rows, rates_row, update_flag = inputs
            widened = block_rows.astype(jnp.float32)
            inverse = lax.rsqrt(lax.optimization_barrier(jnp.sum(widened * widened, axis=1)) / D + EPSILON)
            mixed_rows, updated = layer_group(block_rows, weights, channel_gains[layer_index], rates_row, step_size[layer_index], update_flag, inverse)
            return (updated, mixed_rows)
        rates_blocks = learning_rates[layer_index].reshape(GROUPS, GROUP_TOK)
        flags = update_table[layer_index].astype(jnp.float32)
        last_state, stream = lax.scan(advance, fast_init[layer_index], (stream, rates_blocks, flags))
    return stream.reshape(TOKENS, D)
```

```python
import functools

import jax
import jax.numpy as jnp
from jax import lax
from jax.experimental import pallas as pl
from jax.experimental.pallas import tpu as pltpu
from jax.sharding import PartitionSpec as P

NS_STEPS = 5


MUON_A = 3.4445
MUON_B = -4.775
MUON_C = 2.0315
EPSILON = 1e-06


def passed_along(value, axis, by):
    size = lax.axis_size(axis)
    pairs = [(i, i + by) for i in range(size) if 0 <= i + by < size]
    return lax.ppermute(value, axis, pairs)


def orthogonalize(gradient):
    scaling = lax.rsqrt(jnp.sum(gradient * gradient, axis=(-2, -1), keepdims=True) + EPSILON)
    current = gradient * scaling
    for repeat in range(NS_STEPS):
        square = jnp.einsum("...ij,...kj->...ik", current, current, precision=lax.Precision.HIGHEST)
        polynom = MUON_B * square + MUON_C * jnp.einsum(
            "...ij,...jk->...ik", square, square, precision=lax.Precision.HIGHEST
        )
        current = MUON_A * current + jnp.einsum(
            "...ij,...jk->...ik", polynom, current, precision=lax.Precision.HIGHEST
        )
    return current


def layer_group(stream, entering, gain_rows, rates_row, steps_row, update_flag, inverse):
    row_count, channel_count = stream.shape
    heads_n = entering.shape[1]
    head_dim = entering.shape[2]
    normed = stream.astype(jnp.float32) * inverse[:, None] * gain_rows[0]
    queries = (normed * gain_rows[1]).astype(jnp.bfloat16).reshape(row_count, heads_n, head_dim)
    keys_in = (normed * gain_rows[2]).astype(jnp.bfloat16).reshape(row_count, heads_n, head_dim)
    values_in = (normed * gain_rows[3]).astype(jnp.bfloat16).reshape(row_count, heads_n, head_dim)
    rounded = entering.astype(jnp.bfloat16)
    gate_q = jnp.einsum("thi,hij->thj", queries, rounded[0], preferred_element_type=jnp.float32)
    up_q = jnp.einsum("thi,hij->thj", queries, rounded[1], preferred_element_type=jnp.float32)
    hidden_q = (jax.nn.silu(gate_q) * up_q).astype(jnp.bfloat16)
    output = jnp.einsum(
        "thj,hjk->thk", hidden_q, rounded[2], preferred_element_type=jnp.float32
    ).reshape(row_count, channel_count)
    mixed_rows = (stream.astype(jnp.float32) + gain_rows[4] * output).astype(jnp.bfloat16)
    gate_k = jnp.einsum("thi,hij->thj", keys_in, rounded[0], preferred_element_type=jnp.float32)
    up_k = jnp.einsum("thi,hij->thj", keys_in, rounded[1], preferred_element_type=jnp.float32)
    sigmoid_k = jax.nn.sigmoid(gate_k)
    active_k = gate_k * sigmoid_k
    hidden_k = (active_k * up_k).astype(jnp.bfloat16)
    targets = (rates_row[:, None, None] * values_in.astype(jnp.float32)).astype(jnp.bfloat16)
    back_hidden = jnp.einsum(
        "thk,hjk->thj", targets, rounded[2], preferred_element_type=jnp.float32
    )
    back_up = (back_hidden * active_k).astype(jnp.bfloat16)
    back_gate = (back_hidden * up_k * sigmoid_k * (1.0 + gate_k * (1.0 - sigmoid_k))).astype(
        jnp.bfloat16
    )
    grad_gate = jnp.einsum("thi,thj->hij", keys_in, back_gate, preferred_element_type=jnp.float32)
    grad_up = jnp.einsum("thi,thj->hij", keys_in, back_up, preferred_element_type=jnp.float32)
    grad_down = jnp.einsum("thj,thk->hjk", hidden_k, targets, preferred_element_type=jnp.float32)
    direction = orthogonalize(jnp.stack([grad_gate, grad_up, grad_down]))
    moved_state = entering + (update_flag * steps_row)[None, :, None, None] * direction
    norm_before = jnp.sqrt(jnp.sum(entering * entering, axis=2, keepdims=True) + EPSILON)
    norm_after = jnp.sqrt(jnp.sum(moved_state * moved_state, axis=2, keepdims=True) + EPSILON)
    return (mixed_rows, moved_state * (norm_before / norm_after))


def pass_on(outgoing):
    return passed_along(outgoing, "group", 1)


def body(tokens, learning_rates, channel_gains, fast_init, step_size, update_table):
    start_stream = lax.all_to_all(tokens, "tok", split_axis=1, concat_axis=0, tiled=True)
    group_count = lax.axis_size("group")
    group_index = lax.axis_index("group")
    width_all = start_stream.shape[1] * lax.axis_size("tok")
    layer_count = fast_init.shape[0]
    zero_state = jnp.zeros(fast_init.shape[1:], jnp.float32)

    def tick_work(stream, outgoing, layer_now, active, inverse):
        received = pass_on(outgoing)
        initial = lax.dynamic_index_in_dim(fast_init, layer_now, 0, keepdims=False)
        entering = jnp.where(group_index == 0, initial, received)
        gain_rows = lax.dynamic_index_in_dim(channel_gains, layer_now, 0, keepdims=False)
        rates_row = lax.dynamic_index_in_dim(learning_rates, layer_now, 0, keepdims=False)
        steps_row = lax.dynamic_index_in_dim(step_size, layer_now, 0, keepdims=False)
        table_cell = lax.dynamic_slice(
            update_table, (jnp.asarray(layer_now, jnp.int32), group_index), (1, 1)
        )
        update_flag = table_cell[0, 0].astype(jnp.float32)

        def working(operands):
            return layer_group(
                operands[0], operands[1], gain_rows, rates_row, steps_row, update_flag, inverse
            )

        def resting(operands):
            return (operands[0], operands[2])

        return lax.cond(active, working, resting, (stream, entering, outgoing))

    def one_tick(tick_index, loop_state):
        stream, outgoing = loop_state
        layer_raw = tick_index - group_index
        active = (layer_raw >= 0) & (layer_raw < layer_count)
        layer_now = jnp.clip(layer_raw, 0, layer_count - 1)
        widened = stream.astype(jnp.float32)
        totals = lax.psum(jnp.sum(widened * widened, axis=1), "tok")
        inverse = lax.rsqrt(totals / width_all + EPSILON)
        return tick_work(stream, outgoing, layer_now, active, inverse)

    final_stream, last_state = lax.fori_loop(
        0, layer_count + group_count - 1, one_tick, (start_stream, zero_state)
    )
    return lax.all_to_all(final_stream, "tok", split_axis=0, concat_axis=1, tiled=True)


MESH = pl.DeviceIdType.MESH
F32 = jnp.float32
BF16 = jnp.bfloat16
NN = (((1,), (0,)), ((), ()))
NT = (((1,), (1,)), ((), ()))
TN = (((0,), (0,)), ((), ()))


def dot(a, b, dims=NN):
    return lax.dot_general(a, b, dims, preferred_element_type=F32)


def halves(value):
    high = value.astype(BF16)
    return high, (value - high.astype(F32)).astype(BF16)


def dot3(a, b, dims=NN):
    a_high, a_low = a
    b_high, b_low = b
    return dot(a_high, b_high, dims) + (dot(a_high, b_low, dims) + dot(a_low, b_high, dims))


def sigmoid(value):
    return 0.5 * jnp.tanh(0.5 * value) + 0.5


def newton_schulz(current):
    parts = halves(current)
    square = dot3(parts, parts, NT)
    square_parts = halves(square)
    polynom = MUON_B * square + MUON_C * dot3(square_parts, square_parts)
    return MUON_A * current + dot3(halves(polynom), parts)


def chain_kernel(
    sizes,
    tokens,
    totals,
    rates,
    packed,
    flags,
    initial,
    out,
    xin,
    xout,
    squares,
    sent_squares,
    rate_rows,
    params,
    state,
    columns,
    gate_up,
    down,
    grad_gu,
    grad_d,
    x_recv,
    x_send,
    sq_recv,
    sq_send,
    rate_recv,
    rate_send,
    w_recv,
    w_send,
    p_recv,
    p_send,
    t_send,
    s_send,
    out_recv,
):
    groups, toks, layers, heads, owned, rows, width, tile = sizes
    group_tok = rows * toks
    per = toks // layers
    tiles = group_tok // tile
    tiles_row = rows // tile
    g = lax.axis_index("group")
    t = lax.axis_index("tok")
    me = g * toks + t
    layer = lax.rem(t, layers)
    head = g * per + t // layers
    devices = groups * toks

    def remote(source, target, send, recv, to_g, to_t):
        return pltpu.make_async_remote_copy(
            src_ref=source,
            dst_ref=target,
            send_sem=send,
            recv_sem=recv,
            device_id=(to_g, to_t),
            device_id_type=MESH,
        )

    def deliver(source, target, send, recv, to_g, to_t):
        own = to_g * toks + to_t == me

        @pl.when(own)
        def _():
            pltpu.make_async_copy(source, target, recv).start()

        @pl.when(jnp.logical_not(own))
        def _():
            remote(source, target, send, recv, to_g, to_t).start()

    def sent(source, send, to_g, to_t):
        @pl.when(to_g * toks + to_t != me)
        def _():
            pltpu.make_async_copy(source, source, send).wait()

    def arrived(target, recv):
        pltpu.make_async_copy(target, target, recv).wait()

    barrier = pltpu.get_barrier_semaphore()

    @pl.loop(1, devices)
    def _(step):
        peer = lax.rem(me + step, devices)
        pl.semaphore_signal(
            barrier, inc=1, device_id=(peer // toks, lax.rem(peer, toks)), device_id_type=MESH
        )

    pl.semaphore_wait(barrier, devices - 1)

    def lane(index, size):
        return pl.ds(pl.multiple_of(index * size, size), size)

    def param_of(to_t):
        wanted = g * per + to_t // layers
        return wanted // owned == t, lax.rem(to_t, layers), lax.rem(wanted, owned)

    for to_t in range(toks):
        holds, lay, slot = param_of(to_t)

        @pl.when(holds)
        def _():
            deliver(initial.at[lay, :, slot], state, w_send.at[to_t], w_recv, g, to_t)
            deliver(packed.at[lay, slot], params, p_send.at[to_t], p_recv, g, to_t)

    @pl.loop(0, groups)
    def _(i):
        to_g = lax.rem(g + i, groups)
        deliver(rates.at[layer], rate_rows.at[g], rate_send.at[to_g], rate_recv, to_g, t)

    @pl.loop(0, heads)
    def _(i):
        h = lax.rem(head + i, heads)
        to_g, to_t = h // per, lax.rem(h, per) * layers
        deliver(
            totals, squares.at[g, 0, :, lane(t, rows)], s_send.at[h], sq_recv.at[g], to_g, to_t
        )

    @pl.loop(0, heads)
    def _(i):
        h = lax.rem(head + i, heads)
        to_g, to_t = h // per, lax.rem(h, per) * layers
        deliver(
            tokens.at[:, lane(h, width)],
            xin.at[lane(g * toks + t, rows)],
            t_send.at[h],
            x_recv.at[g, t],
            to_g,
            to_t,
        )

    arrived(state, w_recv)
    arrived(params, p_recv)
    arrived(rate_rows, rate_recv)

    gains = params[...]
    norm_gain = gains[0:1]
    query_gain = norm_gain * gains[1:2]
    key_gain = norm_gain * gains[2:3]
    value_gain = norm_gain * gains[3:4]
    out_gain = gains[4:5]
    step_row = gains[5:6]
    pick_row = lax.broadcasted_iota(jnp.int32, (16, 2 * width), 0)
    pick_lane = lax.broadcasted_iota(jnp.int32, (16, 2 * width), 1)
    spread = jnp.where(pick_row // 2 == pick_lane // width, 1.0, 0.0).astype(BF16)
    ones_rows = jnp.ones((16, width), BF16)

    @pl.loop(0, groups)
    def _(c):
        whole = squares.at[c]

        @pl.when(layer == 0)
        def _():
            arrived(squares.at[c, 0], sq_recv.at[c])
            sent_squares[c] = squares[c, 0]

        @pl.when(layer > 0)
        def _():
            arrived(whole, sq_recv.at[c])
            sent_squares[c] = jnp.sum(squares[c], axis=0)

        inverse = lax.rsqrt(sent_squares[c] / (heads * width) + EPSILON)
        rate = rate_rows[c]
        inverse_high = inverse.astype(BF16).astype(F32)
        rate_high = rate.astype(BF16).astype(F32)
        at_row = lax.broadcasted_iota(jnp.int32, (16, group_tok), 0)
        stack = jnp.where(at_row == 0, inverse_high, 0.0)
        stack = jnp.where(at_row == 1, inverse - inverse_high, stack)
        stack = jnp.where(at_row == 2, rate_high, stack)
        stack = jnp.where(at_row == 3, rate - rate_high, stack)
        columns[...] = dot(stack.astype(BF16), spread, TN)

        gate_up[:, :width] = state[0].astype(BF16)
        gate_up[:, width:] = state[1].astype(BF16)
        down[...] = state[2].astype(BF16)

        @pl.loop(0, toks)
        def _(k):
            arrived(xin.at[lane(c * toks + k, rows)], x_recv.at[c, k])

            @pl.loop(0, tiles_row)
            def _(i):
                at = lane(c * tiles + k * tiles_row + i, tile)
                here = lane(k * tiles_row + i, tile)
                stream = xin[at, :].astype(F32)
                normed = stream * columns[here, :width]
                queries = (normed * query_gain).astype(BF16)
                both = dot(queries, gate_up[...])
                gate = both[:, :width]
                hidden = (gate * sigmoid(gate) * both[:, width:]).astype(BF16)
                mixed = (stream + out_gain * dot(hidden, down[...])).astype(BF16)
                xout[at, :] = mixed
                wide = mixed.astype(F32)
                total = dot(ones_rows, (wide * wide).astype(BF16), NT)
                sent_squares[c, :, here] = total[0:1]

            block = xout.at[lane(c * toks + k, rows)]

            @pl.when(layer < layers - 1)
            def _():
                remote(
                    block,
                    xin.at[lane(c * toks + k, rows)],
                    x_send.at[c, k],
                    x_recv.at[c, k],
                    g,
                    t + 1,
                ).start()

            @pl.when(layer == layers - 1)
            def _():
                deliver(block, out.at[:, lane(head, width)], x_send.at[c, k], out_recv, c, k)

        @pl.when(layer < layers - 1)
        def _():
            @pl.loop(0, heads)
            def _(h):
                remote(
                    sent_squares.at[c],
                    squares.at[c, head],
                    sq_send.at[c],
                    sq_recv.at[c],
                    h // per,
                    lax.rem(h, per) * layers + layer + 1,
                ).start()

        @pl.when(c < groups - 1)
        def _():
            grad_gu[...] = jnp.zeros_like(grad_gu)
            grad_d[...] = jnp.zeros_like(grad_d)

            @pl.loop(0, tiles)
            def _(i):
                at = lane(c * tiles + i, tile)
                here = lane(i, tile)
                scale = columns[here, :]
                normed = xin[at, :].astype(F32) * scale[:, :width]
                keys = (normed * key_gain).astype(BF16)
                values = (normed * value_gain).astype(BF16).astype(F32)
                targets = (values * scale[:, width:]).astype(BF16)
                both = dot(keys, gate_up[...])
                back = dot(targets, down[...], NT)
                gate = both[:, :width]
                up = both[:, width:]
                sig = sigmoid(gate)
                act = gate * sig
                hidden = (act * up).astype(BF16)
                back_up = (back * act).astype(BF16)
                back_gate = (back * up * (sig + act * (1.0 - sig))).astype(BF16)
                grad_gu[...] += dot(keys, jnp.concatenate([back_gate, back_up], axis=1), TN)
                grad_d[...] += dot(hidden, targets, TN)

            grads = (grad_gu[:, :width], grad_gu[:, width:], grad_d[...])
            start = tuple(
                v * lax.rsqrt(jnp.sum(v * v, axis=(0, 1), keepdims=True) + EPSILON) for v in grads
            )
            moves = lax.fori_loop(
                0, NS_STEPS, lambda _, vs: tuple(newton_schulz(v) for v in vs), start
            )
            step = step_row * flags[c]
            for which in range(3):
                entering = state[which]
                moved = entering + step * moves[which]
                before = jnp.sum(entering * entering, axis=0, keepdims=True) + EPSILON
                after = jnp.sum(moved * moved, axis=0, keepdims=True) + EPSILON
                state[which] = moved * (jnp.sqrt(before) * lax.rsqrt(after))

    arrived(out, out_recv)

    for to_t in range(toks):
        holds, lay, slot = param_of(to_t)

        @pl.when(holds)
        def _():
            sent(initial.at[lay, :, slot], w_send.at[to_t], g, to_t)
            sent(packed.at[lay, slot], p_send.at[to_t], g, to_t)

    @pl.loop(0, groups)
    def _(to_g):
        sent(rates.at[layer], rate_send.at[to_g], to_g, t)

        @pl.when(layer < layers - 1)
        def _():
            arrived(squares.at[to_g], sq_send.at[to_g])

        @pl.loop(0, toks)
        def _(k):
            block = xout.at[lane(to_g * toks + k, rows)]

            @pl.when(layer < layers - 1)
            def _():
                arrived(block, x_send.at[to_g, k])

            @pl.when(layer == layers - 1)
            def _():
                sent(block, x_send.at[to_g, k], to_g, k)

    @pl.loop(0, heads)
    def _(h):
        to_g, to_t = h // per, lax.rem(h, per) * layers
        sent(totals, s_send.at[h], to_g, to_t)
        sent(tokens.at[:, lane(h, width)], t_send.at[h], to_g, to_t)


def head_body(tokens, learning_rates, channel_gains, fast_init, step_size, update_table):
    groups, toks = lax.axis_size("group"), lax.axis_size("tok")
    layers, _, owned, width, _ = fast_init.shape
    rows, channels = tokens.shape
    heads = owned * toks
    group_tok = rows * toks
    wide = tokens.astype(F32)
    totals = jnp.sum(wide * wide, axis=1).reshape(1, rows)
    rates = learning_rates.reshape(layers, 1, group_tok)
    gains = channel_gains.reshape(layers, 5, owned, width).transpose(0, 2, 1, 3)
    steps = jnp.broadcast_to(step_size[:, :, None, None], (layers, owned, 3, width))
    packed = jnp.concatenate([gains, steps], axis=2)
    layer = lax.rem(lax.axis_index("tok"), layers)
    flag_row = lax.dynamic_index_in_dim(update_table, layer, 0, keepdims=False).astype(F32)
    flags = jnp.broadcast_to(flag_row[:, None, None], (groups, 1, width))
    tile = 256
    sizes = (groups, toks, layers, heads, owned, rows, width, tile)
    vmem = pl.BlockSpec(memory_space=pltpu.VMEM)
    anywhere = pl.BlockSpec(memory_space=pl.ANY)
    dma = pltpu.SemaphoreType.DMA
    return pl.pallas_call(
        functools.partial(chain_kernel, sizes),
        out_shape=jax.ShapeDtypeStruct((rows, channels), BF16),
        in_specs=[vmem, vmem, vmem, vmem, vmem, anywhere],
        out_specs=anywhere,
        scratch_shapes=[
            pltpu.VMEM((groups * group_tok, width), BF16),
            pltpu.VMEM((groups * group_tok, width), BF16),
            pltpu.VMEM((groups, heads, 1, group_tok), F32),
            pltpu.VMEM((groups, 1, group_tok), F32),
            pltpu.VMEM((groups, 1, group_tok), F32),
            pltpu.VMEM((8, width), F32),
            pltpu.VMEM((3, width, width), F32),
            pltpu.VMEM((group_tok, 2 * width), F32),
            pltpu.VMEM((width, 2 * width), BF16),
            pltpu.VMEM((width, width), BF16),
            pltpu.VMEM((width, 2 * width), F32),
            pltpu.VMEM((width, width), F32),
            dma((groups, toks)),
            dma((groups, toks)),
            dma((groups,)),
            dma((groups,)),
            dma,
            dma((groups,)),
            dma,
            dma((toks,)),
            dma,
            dma((toks,)),
            dma((heads,)),
            dma((heads,)),
            dma,
        ],
        compiler_params=pltpu.CompilerParams(
            collective_id=0, has_side_effects=True, vmem_limit_bytes=48 * 1024 * 1024
        ),
    )(tokens, totals, rates, packed, flags, fast_init)


def plan(mesh, tokens, fast_init):
    groups, toks = mesh.shape["group"], mesh.shape["tok"]
    layers, _, heads, width, _ = fast_init.shape
    rows = tokens.shape[0] // (groups * toks)
    fits = groups * toks == layers * heads and toks % layers == 0 and heads % toks == 0
    fits = fits and rows % 256 == 0 and width % 128 == 0
    return head_body if fits and tokens.shape[0] * width <= 4 * 1024 * 1024 else body


def solution(mesh):
    in_specs = (
        P(("group", "tok"), None),
        P(None, "group"),
        P(None, None, "tok"),
        P(None, None, "tok", None, None),
        P(None, "tok"),
        P(),
    )
    out_specs = P(("group", "tok"), None)
    def run(*args):
        chosen = plan(mesh, args[0], args[3])
        return jax.shard_map(
            chosen, mesh=mesh, in_specs=in_specs, out_specs=out_specs, check_vma=False
        )(*args)

    return run
```

```python
import functools

import jax
import jax.numpy as jnp
from jax import lax
from jax.experimental import pallas as pl
from jax.experimental.pallas import tpu as pltpu
from jax.sharding import PartitionSpec as P

NS_STEPS = 5


MUON_A = 3.4445
MUON_B = -4.775
MUON_C = 2.0315
EPSILON = 1e-06


def passed_along(value, axis, by):
    size = lax.axis_size(axis)
    pairs = [(i, i + by) for i in range(size) if 0 <= i + by < size]
    return lax.ppermute(value, axis, pairs)


def orthogonalize(gradient):
    scaling = lax.rsqrt(jnp.sum(gradient * gradient, axis=(-2, -1), keepdims=True) + EPSILON)
    current = gradient * scaling
    for repeat in range(NS_STEPS):
        square = jnp.einsum("...ij,...kj->...ik", current, current, precision=lax.Precision.HIGHEST)
        polynom = MUON_B * square + MUON_C * jnp.einsum(
            "...ij,...jk->...ik", square, square, precision=lax.Precision.HIGHEST
        )
        current = MUON_A * current + jnp.einsum(
            "...ij,...jk->...ik", polynom, current, precision=lax.Precision.HIGHEST
        )
    return current


def layer_group(stream, entering, gain_rows, rates_row, steps_row, update_flag, inverse):
    row_count, channel_count = stream.shape
    heads_n = entering.shape[1]
    head_dim = entering.shape[2]
    normed = stream.astype(jnp.float32) * inverse[:, None] * gain_rows[0]
    queries = (normed * gain_rows[1]).astype(jnp.bfloat16).reshape(row_count, heads_n, head_dim)
    keys_in = (normed * gain_rows[2]).astype(jnp.bfloat16).reshape(row_count, heads_n, head_dim)
    values_in = (normed * gain_rows[3]).astype(jnp.bfloat16).reshape(row_count, heads_n, head_dim)
    rounded = entering.astype(jnp.bfloat16)
    gate_q = jnp.einsum("thi,hij->thj", queries, rounded[0], preferred_element_type=jnp.float32)
    up_q = jnp.einsum("thi,hij->thj", queries, rounded[1], preferred_element_type=jnp.float32)
    hidden_q = (jax.nn.silu(gate_q) * up_q).astype(jnp.bfloat16)
    output = jnp.einsum(
        "thj,hjk->thk", hidden_q, rounded[2], preferred_element_type=jnp.float32
    ).reshape(row_count, channel_count)
    mixed_rows = (stream.astype(jnp.float32) + gain_rows[4] * output).astype(jnp.bfloat16)
    gate_k = jnp.einsum("thi,hij->thj", keys_in, rounded[0], preferred_element_type=jnp.float32)
    up_k = jnp.einsum("thi,hij->thj", keys_in, rounded[1], preferred_element_type=jnp.float32)
    sigmoid_k = jax.nn.sigmoid(gate_k)
    active_k = gate_k * sigmoid_k
    hidden_k = (active_k * up_k).astype(jnp.bfloat16)
    targets = (rates_row[:, None, None] * values_in.astype(jnp.float32)).astype(jnp.bfloat16)
    back_hidden = jnp.einsum(
        "thk,hjk->thj", targets, rounded[2], preferred_element_type=jnp.float32
    )
    back_up = (back_hidden * active_k).astype(jnp.bfloat16)
    back_gate = (back_hidden * up_k * sigmoid_k * (1.0 + gate_k * (1.0 - sigmoid_k))).astype(
        jnp.bfloat16
    )
    grad_gate = jnp.einsum("thi,thj->hij", keys_in, back_gate, preferred_element_type=jnp.float32)
    grad_up = jnp.einsum("thi,thj->hij", keys_in, back_up, preferred_element_type=jnp.float32)
    grad_down = jnp.einsum("thj,thk->hjk", hidden_k, targets, preferred_element_type=jnp.float32)
    direction = orthogonalize(jnp.stack([grad_gate, grad_up, grad_down]))
    moved_state = entering + (update_flag * steps_row)[None, :, None, None] * direction
    norm_before = jnp.sqrt(jnp.sum(entering * entering, axis=2, keepdims=True) + EPSILON)
    norm_after = jnp.sqrt(jnp.sum(moved_state * moved_state, axis=2, keepdims=True) + EPSILON)
    return (mixed_rows, moved_state * (norm_before / norm_after))


def pass_on(outgoing):
    return passed_along(outgoing, "group", 1)


def body(tokens, learning_rates, channel_gains, fast_init, step_size, update_table):
    start_stream = lax.all_to_all(tokens, "tok", split_axis=1, concat_axis=0, tiled=True)
    group_count = lax.axis_size("group")
    group_index = lax.axis_index("group")
    width_all = start_stream.shape[1] * lax.axis_size("tok")
    layer_count = fast_init.shape[0]
    zero_state = jnp.zeros(fast_init.shape[1:], jnp.float32)

    def tick_work(stream, outgoing, layer_now, active, inverse):
        received = pass_on(outgoing)
        initial = lax.dynamic_index_in_dim(fast_init, layer_now, 0, keepdims=False)
        entering = jnp.where(group_index == 0, initial, received)
        gain_rows = lax.dynamic_index_in_dim(channel_gains, layer_now, 0, keepdims=False)
        rates_row = lax.dynamic_index_in_dim(learning_rates, layer_now, 0, keepdims=False)
        steps_row = lax.dynamic_index_in_dim(step_size, layer_now, 0, keepdims=False)
        table_cell = lax.dynamic_slice(
            update_table, (jnp.asarray(layer_now, jnp.int32), group_index), (1, 1)
        )
        update_flag = table_cell[0, 0].astype(jnp.float32)

        def working(operands):
            return layer_group(
                operands[0], operands[1], gain_rows, rates_row, steps_row, update_flag, inverse
            )

        def resting(operands):
            return (operands[0], operands[2])

        return lax.cond(active, working, resting, (stream, entering, outgoing))

    def one_tick(tick_index, loop_state):
        stream, outgoing = loop_state
        layer_raw = tick_index - group_index
        active = (layer_raw >= 0) & (layer_raw < layer_count)
        layer_now = jnp.clip(layer_raw, 0, layer_count - 1)
        widened = stream.astype(jnp.float32)
        totals = lax.psum(jnp.sum(widened * widened, axis=1), "tok")
        inverse = lax.rsqrt(totals / width_all + EPSILON)
        return tick_work(stream, outgoing, layer_now, active, inverse)

    final_stream, last_state = lax.fori_loop(
        0, layer_count + group_count - 1, one_tick, (start_stream, zero_state)
    )
    return lax.all_to_all(final_stream, "tok", split_axis=0, concat_axis=1, tiled=True)


MESH = pl.DeviceIdType.MESH
F32 = jnp.float32
BF16 = jnp.bfloat16
NN = (((1,), (0,)), ((), ()))
NT = (((1,), (1,)), ((), ()))
TN = (((0,), (0,)), ((), ()))


def dot(a, b, dims=NN):
    return lax.dot_general(a, b, dims, preferred_element_type=F32)


def halves(value):
    high = value.astype(BF16)
    return high, (value - high.astype(F32)).astype(BF16)


def product(a, b):
    a_high, a_low = halves(a)
    b_high, b_low = halves(b)
    left = jnp.concatenate([a_high, a_low], axis=1)
    above = jnp.concatenate([b_high, b_low], axis=1)
    below = jnp.concatenate([b_high, jnp.zeros_like(b_low)], axis=1)
    both = dot(left, jnp.concatenate([above, below], axis=0))
    return both[:, : b.shape[1]] + both[:, b.shape[1] :]


def gram(a):
    high, low = halves(a)
    left = jnp.concatenate([high, low], axis=1)
    above = jnp.concatenate([high, high], axis=1)
    below = jnp.concatenate([low, jnp.zeros_like(low)], axis=1)
    both = dot(left, jnp.concatenate([above, below], axis=0), NT)
    return both[:, : a.shape[0]] + both[:, a.shape[0] :]


def sigmoid(value):
    return 0.5 * jnp.tanh(0.5 * value) + 0.5


def newton_schulz(values):
    squares = [gram(v) for v in values]
    polynoms = [MUON_B * q + MUON_C * product(q, q) for q in squares]
    return tuple(MUON_A * v + product(p, v) for p, v in zip(polynoms, values))


def chain_kernel(
    sizes,
    tokens,
    rates,
    packed,
    flags,
    initial,
    out,
    xin,
    xout,
    squares,
    sent_squares,
    rate_rows,
    params,
    state,
    totals,
    stack,
    gate_up,
    down,
    grad_gu,
    grad_d,
    x_recv,
    x_send,
    sq_recv,
    sq_send,
    rate_recv,
    rate_send,
    w_recv,
    w_send,
    p_recv,
    p_send,
    t_send,
    s_send,
    out_recv,
):
    groups, toks, layers, heads, owned, rows, width, tile = sizes
    group_tok = rows * toks
    per = toks // layers
    tiles = group_tok // tile
    tiles_row = rows // tile
    g = lax.axis_index("group")
    t = lax.axis_index("tok")
    me = g * toks + t
    layer = lax.rem(t, layers)
    head = g * per + t // layers
    devices = groups * toks

    def remote(source, target, send, recv, to_g, to_t):
        return pltpu.make_async_remote_copy(
            src_ref=source,
            dst_ref=target,
            send_sem=send,
            recv_sem=recv,
            device_id=(to_g, to_t),
            device_id_type=MESH,
        )

    def deliver(source, target, send, recv, to_g, to_t):
        own = to_g * toks + to_t == me

        @pl.when(own)
        def _():
            pltpu.make_async_copy(source, target, recv).start()

        @pl.when(jnp.logical_not(own))
        def _():
            remote(source, target, send, recv, to_g, to_t).start()

    def sent(source, send, to_g, to_t):
        @pl.when(to_g * toks + to_t != me)
        def _():
            pltpu.make_async_copy(source, source, send).wait()

    def arrived(target, recv):
        pltpu.make_async_copy(target, target, recv).wait()

    barrier = pltpu.get_barrier_semaphore()

    @pl.loop(1, devices)
    def _(step):
        peer = lax.rem(me + step, devices)
        pl.semaphore_signal(
            barrier, inc=1, device_id=(peer // toks, lax.rem(peer, toks)), device_id_type=MESH
        )

    pl.semaphore_wait(barrier, devices - 1)

    def lane(index, size):
        return pl.ds(pl.multiple_of(index * size, size), size)

    def param_of(to_t):
        wanted = g * per + to_t // layers
        return wanted // owned == t, lax.rem(to_t, layers), lax.rem(wanted, owned)

    for to_t in range(toks):
        holds, lay, slot = param_of(to_t)

        @pl.when(holds)
        def _():
            deliver(initial.at[lay, :, slot], state, w_send.at[to_t], w_recv, g, to_t)
            deliver(packed.at[lay, slot], params, p_send.at[to_t], p_recv, g, to_t)

    @pl.loop(0, groups)
    def _(i):
        to_g = lax.rem(g + i, groups)
        deliver(rates.at[layer], rate_rows.at[g], rate_send.at[to_g], rate_recv, to_g, t)

    @pl.loop(0, heads)
    def _(i):
        h = lax.rem(head + i, heads)
        to_g, to_t = h // per, lax.rem(h, per) * layers
        deliver(
            tokens.at[:, lane(h, width)],
            xin.at[lane(g * toks + t, rows)],
            t_send.at[h],
            x_recv.at[g, t],
            to_g,
            to_t,
        )

    ones_rows = jnp.ones((16, width), BF16)

    def sums_of(values):
        wide = values.astype(F32)
        return dot(ones_rows, (wide * wide).astype(BF16), NT)[0:1]

    totals[...] = jnp.zeros_like(totals)

    @pl.loop(0, heads)
    def _(h):
        totals[...] += sums_of(tokens[:, lane(h, width)])

    @pl.loop(0, heads)
    def _(i):
        h = lax.rem(head + i, heads)
        to_g, to_t = h // per, lax.rem(h, per) * layers
        deliver(
            totals, squares.at[g, 0, :, lane(t, rows)], s_send.at[h], sq_recv.at[g], to_g, to_t
        )

    arrived(state, w_recv)
    arrived(params, p_recv)
    arrived(rate_rows, rate_recv)

    gains = params[...]
    norm_gain = gains[0:1]
    query_gain = norm_gain * gains[1:2]
    key_gain = norm_gain * gains[2:3]
    value_gain = norm_gain * gains[3:4]
    out_gain = gains[4:5]
    step_row = gains[5:6]
    pick_row = lax.broadcasted_iota(jnp.int32, (16, 2 * width), 0)
    pick_lane = lax.broadcasted_iota(jnp.int32, (16, 2 * width), 1)
    spread = jnp.where(pick_row // 2 == pick_lane // width, 1.0, 0.0).astype(BF16)
    @pl.loop(0, groups)
    def _(c):
        whole = squares.at[c]

        @pl.when(layer == 0)
        def _():
            arrived(squares.at[c, 0], sq_recv.at[c])
            sent_squares[c] = squares[c, 0]

        @pl.when(layer > 0)
        def _():
            arrived(whole, sq_recv.at[c])
            sent_squares[c] = jnp.sum(squares[c], axis=0)

        inverse = lax.rsqrt(sent_squares[c] / (heads * width) + EPSILON)
        rate = rate_rows[c]
        inverse_high = inverse.astype(BF16).astype(F32)
        rate_high = rate.astype(BF16).astype(F32)
        at_row = lax.broadcasted_iota(jnp.int32, (16, group_tok), 0)
        fill = jnp.where(at_row == 0, inverse_high, 0.0)
        fill = jnp.where(at_row == 1, inverse - inverse_high, fill)
        fill = jnp.where(at_row == 2, rate_high, fill)
        stack[...] = jnp.where(at_row == 3, rate - rate_high, fill).astype(BF16)

        gate_up[:, :width] = state[0].astype(BF16)
        gate_up[:, width:] = state[1].astype(BF16)
        down[...] = state[2].astype(BF16)

        def read(i):
            at = lane(c * tiles + i, tile)
            here = lane(i, tile)

            def query():
                stream = xin[at, :].astype(F32)
                normed = stream * dot(stack[:, here], spread[:, :width], TN)
                queries = (normed * query_gain).astype(BF16)
                both = dot(queries, gate_up[...])
                gate = both[:, :width]
                hidden = (gate * sigmoid(gate) * both[:, width:]).astype(BF16)
                mixed = (stream + out_gain * dot(hidden, down[...])).astype(BF16)
                xout[at, :] = mixed
                sent_squares[c, :, here] = sums_of(mixed)

            def learn():
                scale = dot(stack[:, here], spread, TN)
                normed = xin[at, :].astype(F32) * scale[:, :width]
                keys = (normed * key_gain).astype(BF16)
                targets = (normed * value_gain * scale[:, width:]).astype(BF16)
                both = dot(keys, gate_up[...])
                back = dot(targets, down[...], NT)
                gate = both[:, :width]
                up = both[:, width:]
                sig = sigmoid(gate)
                act = gate * sig
                hidden = (act * up).astype(BF16)
                back_up = (back * act).astype(BF16)
                back_gate = (back * up * (sig + act * (1.0 - sig))).astype(BF16)
                backs = jnp.concatenate([back_gate, back_up], axis=1)
                return dot(keys, backs, TN), dot(hidden, targets, TN)

            return query, learn

        def answer(k):
            for i in range(tiles_row):
                read(k * tiles_row + i)[0]()

        def await_rows(k):
            arrived(xin.at[lane(c * toks + k, rows)], x_recv.at[c, k])

        def send_rows(k):
            block = xout.at[lane(c * toks + k, rows)]

            @pl.when(layer < layers - 1)
            def _():
                remote(
                    block,
                    xin.at[lane(c * toks + k, rows)],
                    x_send.at[c, k],
                    x_recv.at[c, k],
                    g,
                    t + 1,
                ).start()

            @pl.when(layer == layers - 1)
            def _():
                deliver(block, out.at[:, lane(head, width)], x_send.at[c, k], out_recv, c, k)

        def send_squares():
            @pl.when(layer < layers - 1)
            def _():
                @pl.loop(0, heads)
                def _(h):
                    remote(
                        sent_squares.at[c],
                        squares.at[c, head],
                        sq_send.at[c],
                        sq_recv.at[c],
                        h // per,
                        lax.rem(h, per) * layers + layer + 1,
                    ).start()

        @pl.when(c == groups - 1)
        def _():
            @pl.loop(0, toks)
            def _(k):
                await_rows(k)
                answer(k)
                send_rows(k)

            send_squares()

        @pl.when(c < groups - 1)
        def _():
            grad_gu[...] = jnp.zeros_like(grad_gu)
            grad_d[...] = jnp.zeros_like(grad_d)

            @pl.loop(0, toks)
            def _(k):
                await_rows(k)
                found = [read(k * tiles_row + i)[1]() for i in range(tiles_row)]
                grad_gu[...] += sum(f[0] for f in found)
                grad_d[...] += sum(f[1] for f in found)

            grads = (grad_gu[:, :width], grad_gu[:, width:], grad_d[...])
            start = tuple(
                v * lax.rsqrt(jnp.sum(v * v, axis=(0, 1), keepdims=True) + EPSILON) for v in grads
            )

            def beside(k, values):
                answer(k)
                values = newton_schulz(values)
                send_rows(k)
                return values

            moves = lax.fori_loop(0, toks, beside, start)
            send_squares()
            for _ in range(NS_STEPS - toks):
                moves = newton_schulz(moves)
            step = step_row * flags[c]
            for which in range(3):
                entering = state[which]
                moved = entering + step * moves[which]
                before = jnp.sum(entering * entering, axis=0, keepdims=True) + EPSILON
                after = jnp.sum(moved * moved, axis=0, keepdims=True) + EPSILON
                state[which] = moved * (jnp.sqrt(before) * lax.rsqrt(after))

    arrived(out, out_recv)

    for to_t in range(toks):
        holds, lay, slot = param_of(to_t)

        @pl.when(holds)
        def _():
            sent(initial.at[lay, :, slot], w_send.at[to_t], g, to_t)
            sent(packed.at[lay, slot], p_send.at[to_t], g, to_t)

    @pl.loop(0, groups)
    def _(to_g):
        sent(rates.at[layer], rate_send.at[to_g], to_g, t)

        @pl.when(layer < layers - 1)
        def _():
            arrived(squares.at[to_g], sq_send.at[to_g])

        @pl.loop(0, toks)
        def _(k):
            block = xout.at[lane(to_g * toks + k, rows)]

            @pl.when(layer < layers - 1)
            def _():
                arrived(block, x_send.at[to_g, k])

            @pl.when(layer == layers - 1)
            def _():
                sent(block, x_send.at[to_g, k], to_g, k)

    @pl.loop(0, heads)
    def _(h):
        to_g, to_t = h // per, lax.rem(h, per) * layers
        sent(totals, s_send.at[h], to_g, to_t)
        sent(tokens.at[:, lane(h, width)], t_send.at[h], to_g, to_t)


def head_body(tokens, learning_rates, channel_gains, fast_init, step_size, update_table):
    groups, toks = lax.axis_size("group"), lax.axis_size("tok")
    layers, _, owned, width, _ = fast_init.shape
    rows, channels = tokens.shape
    heads = owned * toks
    group_tok = rows * toks
    rates = learning_rates.reshape(layers, 1, group_tok)
    gains = channel_gains.reshape(layers, 5, owned, width).transpose(0, 2, 1, 3)
    steps = jnp.broadcast_to(step_size[:, :, None, None], (layers, owned, 3, width))
    packed = jnp.concatenate([gains, steps], axis=2)
    layer = lax.rem(lax.axis_index("tok"), layers)
    flag_row = lax.dynamic_index_in_dim(update_table, layer, 0, keepdims=False).astype(F32)
    flags = jnp.broadcast_to(flag_row[:, None, None], (groups, 1, width))
    tile = 256
    sizes = (groups, toks, layers, heads, owned, rows, width, tile)
    vmem = pl.BlockSpec(memory_space=pltpu.VMEM)
    anywhere = pl.BlockSpec(memory_space=pl.ANY)
    dma = pltpu.SemaphoreType.DMA
    return pl.pallas_call(
        functools.partial(chain_kernel, sizes),
        out_shape=jax.ShapeDtypeStruct((rows, channels), BF16),
        in_specs=[vmem, vmem, vmem, vmem, anywhere],
        out_specs=anywhere,
        scratch_shapes=[
            pltpu.VMEM((groups * group_tok, width), BF16),
            pltpu.VMEM((groups * group_tok, width), BF16),
            pltpu.VMEM((groups, heads, 1, group_tok), F32),
            pltpu.VMEM((groups, 1, group_tok), F32),
            pltpu.VMEM((groups, 1, group_tok), F32),
            pltpu.VMEM((8, width), F32),
            pltpu.VMEM((3, width, width), F32),
            pltpu.VMEM((1, rows), F32),
            pltpu.VMEM((16, group_tok), BF16),
            pltpu.VMEM((width, 2 * width), BF16),
            pltpu.VMEM((width, width), BF16),
            pltpu.VMEM((width, 2 * width), F32),
            pltpu.VMEM((width, width), F32),
            dma((groups, toks)),
            dma((groups, toks)),
            dma((groups,)),
            dma((groups,)),
            dma,
            dma((groups,)),
            dma,
            dma((toks,)),
            dma,
            dma((toks,)),
            dma((heads,)),
            dma((heads,)),
            dma,
        ],
        compiler_params=pltpu.CompilerParams(
            collective_id=0, has_side_effects=True, vmem_limit_bytes=48 * 1024 * 1024
        ),
    )(tokens, rates, packed, flags, fast_init)


def plan(mesh, tokens, fast_init):
    groups, toks = mesh.shape["group"], mesh.shape["tok"]
    layers, _, heads, width, _ = fast_init.shape
    rows = tokens.shape[0] // (groups * toks)
    fits = groups * toks == layers * heads and toks % layers == 0 and heads % toks == 0
    fits = fits and toks <= NS_STEPS and rows % 256 == 0 and width % 128 == 0
    return head_body if fits and tokens.shape[0] * width <= 4 * 1024 * 1024 else body


def solution(mesh):
    in_specs = (
        P(("group", "tok"), None),
        P(None, "group"),
        P(None, None, "tok"),
        P(None, None, "tok", None, None),
        P(None, "tok"),
        P(),
    )
    out_specs = P(("group", "tok"), None)
    def run(*args):
        chosen = plan(mesh, args[0], args[3])
        return jax.shard_map(
            chosen, mesh=mesh, in_specs=in_specs, out_specs=out_specs, check_vma=False
        )(*args)

    return run
```

```python
import functools

import jax
import jax.numpy as jnp
from jax import lax
from jax.experimental import pallas as pl
from jax.experimental.pallas import tpu as pltpu
from jax.sharding import PartitionSpec as P

NS_STEPS = 5


MUON_A = 3.4445
MUON_B = -4.775
MUON_C = 2.0315
EPSILON = 1e-06


def passed_along(value, axis, by):
    size = lax.axis_size(axis)
    pairs = [(i, i + by) for i in range(size) if 0 <= i + by < size]
    return lax.ppermute(value, axis, pairs)


def orthogonalize(gradient):
    scaling = lax.rsqrt(jnp.sum(gradient * gradient, axis=(-2, -1), keepdims=True) + EPSILON)
    current = gradient * scaling
    for repeat in range(NS_STEPS):
        square = jnp.einsum("...ij,...kj->...ik", current, current, precision=lax.Precision.HIGHEST)
        polynom = MUON_B * square + MUON_C * jnp.einsum(
            "...ij,...jk->...ik", square, square, precision=lax.Precision.HIGHEST
        )
        current = MUON_A * current + jnp.einsum(
            "...ij,...jk->...ik", polynom, current, precision=lax.Precision.HIGHEST
        )
    return current


def layer_group(stream, entering, gain_rows, rates_row, steps_row, update_flag, inverse):
    row_count, channel_count = stream.shape
    heads_n = entering.shape[1]
    head_dim = entering.shape[2]
    normed = stream.astype(jnp.float32) * inverse[:, None] * gain_rows[0]
    queries = (normed * gain_rows[1]).astype(jnp.bfloat16).reshape(row_count, heads_n, head_dim)
    keys_in = (normed * gain_rows[2]).astype(jnp.bfloat16).reshape(row_count, heads_n, head_dim)
    values_in = (normed * gain_rows[3]).astype(jnp.bfloat16).reshape(row_count, heads_n, head_dim)
    rounded = entering.astype(jnp.bfloat16)
    gate_q = jnp.einsum("thi,hij->thj", queries, rounded[0], preferred_element_type=jnp.float32)
    up_q = jnp.einsum("thi,hij->thj", queries, rounded[1], preferred_element_type=jnp.float32)
    hidden_q = (jax.nn.silu(gate_q) * up_q).astype(jnp.bfloat16)
    output = jnp.einsum(
        "thj,hjk->thk", hidden_q, rounded[2], preferred_element_type=jnp.float32
    ).reshape(row_count, channel_count)
    mixed_rows = (stream.astype(jnp.float32) + gain_rows[4] * output).astype(jnp.bfloat16)
    gate_k = jnp.einsum("thi,hij->thj", keys_in, rounded[0], preferred_element_type=jnp.float32)
    up_k = jnp.einsum("thi,hij->thj", keys_in, rounded[1], preferred_element_type=jnp.float32)
    sigmoid_k = jax.nn.sigmoid(gate_k)
    active_k = gate_k * sigmoid_k
    hidden_k = (active_k * up_k).astype(jnp.bfloat16)
    targets = (rates_row[:, None, None] * values_in.astype(jnp.float32)).astype(jnp.bfloat16)
    back_hidden = jnp.einsum(
        "thk,hjk->thj", targets, rounded[2], preferred_element_type=jnp.float32
    )
    back_up = (back_hidden * active_k).astype(jnp.bfloat16)
    back_gate = (back_hidden * up_k * sigmoid_k * (1.0 + gate_k * (1.0 - sigmoid_k))).astype(
        jnp.bfloat16
    )
    grad_gate = jnp.einsum("thi,thj->hij", keys_in, back_gate, preferred_element_type=jnp.float32)
    grad_up = jnp.einsum("thi,thj->hij", keys_in, back_up, preferred_element_type=jnp.float32)
    grad_down = jnp.einsum("thj,thk->hjk", hidden_k, targets, preferred_element_type=jnp.float32)
    direction = orthogonalize(jnp.stack([grad_gate, grad_up, grad_down]))
    moved_state = entering + (update_flag * steps_row)[None, :, None, None] * direction
    norm_before = jnp.sqrt(jnp.sum(entering * entering, axis=2, keepdims=True) + EPSILON)
    norm_after = jnp.sqrt(jnp.sum(moved_state * moved_state, axis=2, keepdims=True) + EPSILON)
    return (mixed_rows, moved_state * (norm_before / norm_after))


def pass_on(outgoing):
    return passed_along(outgoing, "group", 1)


def body(tokens, learning_rates, channel_gains, fast_init, step_size, update_table):
    start_stream = lax.all_to_all(tokens, "tok", split_axis=1, concat_axis=0, tiled=True)
    group_count = lax.axis_size("group")
    group_index = lax.axis_index("group")
    width_all = start_stream.shape[1] * lax.axis_size("tok")
    layer_count = fast_init.shape[0]
    zero_state = jnp.zeros(fast_init.shape[1:], jnp.float32)

    def tick_work(stream, outgoing, layer_now, active, inverse):
        received = pass_on(outgoing)
        initial = lax.dynamic_index_in_dim(fast_init, layer_now, 0, keepdims=False)
        entering = jnp.where(group_index == 0, initial, received)
        gain_rows = lax.dynamic_index_in_dim(channel_gains, layer_now, 0, keepdims=False)
        rates_row = lax.dynamic_index_in_dim(learning_rates, layer_now, 0, keepdims=False)
        steps_row = lax.dynamic_index_in_dim(step_size, layer_now, 0, keepdims=False)
        table_cell = lax.dynamic_slice(
            update_table, (jnp.asarray(layer_now, jnp.int32), group_index), (1, 1)
        )
        update_flag = table_cell[0, 0].astype(jnp.float32)

        def working(operands):
            return layer_group(
                operands[0], operands[1], gain_rows, rates_row, steps_row, update_flag, inverse
            )

        def resting(operands):
            return (operands[0], operands[2])

        return lax.cond(active, working, resting, (stream, entering, outgoing))

    def one_tick(tick_index, loop_state):
        stream, outgoing = loop_state
        layer_raw = tick_index - group_index
        active = (layer_raw >= 0) & (layer_raw < layer_count)
        layer_now = jnp.clip(layer_raw, 0, layer_count - 1)
        widened = stream.astype(jnp.float32)
        totals = lax.psum(jnp.sum(widened * widened, axis=1), "tok")
        inverse = lax.rsqrt(totals / width_all + EPSILON)
        return tick_work(stream, outgoing, layer_now, active, inverse)

    final_stream, last_state = lax.fori_loop(
        0, layer_count + group_count - 1, one_tick, (start_stream, zero_state)
    )
    return lax.all_to_all(final_stream, "tok", split_axis=0, concat_axis=1, tiled=True)


MESH = pl.DeviceIdType.MESH
F32 = jnp.float32
BF16 = jnp.bfloat16
NN = (((1,), (0,)), ((), ()))
NT = (((1,), (1,)), ((), ()))
TN = (((0,), (0,)), ((), ()))


def dot(a, b, dims=NN):
    return lax.dot_general(a, b, dims, preferred_element_type=F32)


def halves(value):
    high = value.astype(BF16)
    return high, (value - high.astype(F32)).astype(BF16)


def product(a, b):
    a_high, a_low = halves(a)
    b_high, b_low = halves(b)
    left = jnp.concatenate([a_high, a_low], axis=1)
    above = jnp.concatenate([b_high, b_low], axis=1)
    below = jnp.concatenate([b_high, jnp.zeros_like(b_low)], axis=1)
    both = dot(left, jnp.concatenate([above, below], axis=0))
    return both[:, : b.shape[1]] + both[:, b.shape[1] :]


def gram(a):
    high, low = halves(a)
    left = jnp.concatenate([high, low], axis=1)
    above = jnp.concatenate([high, high], axis=1)
    below = jnp.concatenate([low, jnp.zeros_like(low)], axis=1)
    both = dot(left, jnp.concatenate([above, below], axis=0), NT)
    return both[:, : a.shape[0]] + both[:, a.shape[0] :]


def sigmoid(value):
    return 0.5 * jnp.tanh(0.5 * value) + 0.5


def newton_schulz(values):
    squares = [gram(v) for v in values]
    polynoms = [MUON_B * q + MUON_C * product(q, q) for q in squares]
    return tuple(MUON_A * v + product(p, v) for p, v in zip(polynoms, values))


def chain_kernel(
    sizes,
    tokens,
    rates,
    packed,
    flags,
    initial,
    out,
    xin,
    xout,
    squares,
    sent_squares,
    rate_rows,
    params,
    state,
    totals,
    stack,
    gate_up,
    down,
    grad_gu,
    grad_d,
    x_recv,
    x_send,
    sq_recv,
    sq_send,
    rate_recv,
    rate_send,
    w_recv,
    w_send,
    p_recv,
    p_send,
    t_send,
    s_send,
    out_recv,
):
    groups, toks, layers, heads, owned, rows, width, tile = sizes
    group_tok = rows * toks
    per = toks // layers
    tiles = group_tok // tile
    tiles_row = rows // tile
    g = lax.axis_index("group")
    t = lax.axis_index("tok")
    me = g * toks + t
    layer = lax.rem(t, layers)
    head = g * per + t // layers
    devices = groups * toks

    def remote(source, target, send, recv, to_g, to_t):
        return pltpu.make_async_remote_copy(
            src_ref=source,
            dst_ref=target,
            send_sem=send,
            recv_sem=recv,
            device_id=(to_g, to_t),
            device_id_type=MESH,
        )

    def deliver(source, target, send, recv, to_g, to_t):
        own = to_g * toks + to_t == me

        @pl.when(own)
        def _():
            pltpu.make_async_copy(source, target, recv).start()

        @pl.when(jnp.logical_not(own))
        def _():
            remote(source, target, send, recv, to_g, to_t).start()

    def sent(source, send, to_g, to_t):
        @pl.when(to_g * toks + to_t != me)
        def _():
            pltpu.make_async_copy(source, source, send).wait()

    def arrived(target, recv):
        pltpu.make_async_copy(target, target, recv).wait()

    barrier = pltpu.get_barrier_semaphore()

    @pl.loop(1, devices)
    def _(step):
        peer = lax.rem(me + step, devices)
        pl.semaphore_signal(
            barrier, inc=1, device_id=(peer // toks, lax.rem(peer, toks)), device_id_type=MESH
        )

    pl.semaphore_wait(barrier, devices - 1)

    def lane(index, size):
        return pl.ds(pl.multiple_of(index * size, size), size)

    def param_of(to_t):
        wanted = g * per + to_t // layers
        return wanted // owned == t, lax.rem(to_t, layers), lax.rem(wanted, owned)

    for to_t in range(toks):
        holds, lay, slot = param_of(to_t)

        @pl.when(holds)
        def _():
            deliver(initial.at[lay, :, slot], state, w_send.at[to_t], w_recv, g, to_t)
            deliver(packed.at[lay, slot], params, p_send.at[to_t], p_recv, g, to_t)

    @pl.loop(0, groups)
    def _(i):
        to_g = lax.rem(g + i, groups)
        deliver(rates.at[layer], rate_rows.at[g], rate_send.at[to_g], rate_recv, to_g, t)

    @pl.loop(0, heads)
    def _(i):
        h = lax.rem(head + i, heads)
        to_g, to_t = h // per, lax.rem(h, per) * layers
        deliver(
            tokens.at[:, lane(h, width)],
            xin.at[lane(g * toks + t, rows)],
            t_send.at[h],
            x_recv.at[g, t],
            to_g,
            to_t,
        )

    ones_rows = jnp.ones((16, width), BF16)

    def sums_of(values):
        wide = values.astype(F32)
        return dot(ones_rows, (wide * wide).astype(BF16), NT)[0:1]

    totals[...] = jnp.zeros_like(totals)

    @pl.loop(0, heads)
    def _(h):
        totals[...] += sums_of(tokens[:, lane(h, width)])

    @pl.loop(0, heads)
    def _(i):
        h = lax.rem(head + i, heads)
        to_g, to_t = h // per, lax.rem(h, per) * layers
        deliver(
            totals, squares.at[g, 0, :, lane(t, rows)], s_send.at[h], sq_recv.at[g], to_g, to_t
        )

    arrived(state, w_recv)
    arrived(params, p_recv)
    arrived(rate_rows, rate_recv)

    gains = params[...]
    norm_gain = gains[0:1]
    query_gain = norm_gain * gains[1:2]
    key_gain = norm_gain * gains[2:3]
    value_gain = norm_gain * gains[3:4]
    out_gain = gains[4:5]
    step_row = gains[5:6]
    pick_row = lax.broadcasted_iota(jnp.int32, (16, 2 * width), 0)
    pick_lane = lax.broadcasted_iota(jnp.int32, (16, 2 * width), 1)
    spread = jnp.where(pick_row // 2 == pick_lane // width, 1.0, 0.0).astype(BF16)
    @pl.loop(0, groups)
    def _(c):
        whole = squares.at[c]

        @pl.when(layer == 0)
        def _():
            arrived(squares.at[c, 0], sq_recv.at[c])
            sent_squares[c] = squares[c, 0]

        @pl.when(layer > 0)
        def _():
            arrived(whole, sq_recv.at[c])
            sent_squares[c] = jnp.sum(squares[c], axis=0)

        inverse = lax.rsqrt(sent_squares[c] / (heads * width) + EPSILON)
        rate = rate_rows[c]
        inverse_high = inverse.astype(BF16).astype(F32)
        rate_high = rate.astype(BF16).astype(F32)
        at_row = lax.broadcasted_iota(jnp.int32, (16, group_tok), 0)
        fill = jnp.where(at_row == 0, inverse_high, 0.0)
        fill = jnp.where(at_row == 1, inverse - inverse_high, fill)
        fill = jnp.where(at_row == 2, rate_high, fill)
        stack[...] = jnp.where(at_row == 3, rate - rate_high, fill).astype(BF16)

        gate_up[:, :width] = state[0].astype(BF16)
        gate_up[:, width:] = state[1].astype(BF16)
        down[...] = state[2].astype(BF16)

        def read(i):
            at = lane(c * tiles + i, tile)
            here = lane(i, tile)

            def query():
                stream = xin[at, :].astype(F32)
                normed = stream * dot(stack[:, here], spread[:, :width], TN)
                queries = (normed * query_gain).astype(BF16)
                both = dot(queries, gate_up[...])
                gate = both[:, :width]
                hidden = (gate * sigmoid(gate) * both[:, width:]).astype(BF16)
                mixed = (stream + out_gain * dot(hidden, down[...])).astype(BF16)
                xout[at, :] = mixed
                sent_squares[c, :, here] = sums_of(mixed)

            def learn():
                scale = dot(stack[:, here], spread, TN)
                normed = xin[at, :].astype(F32) * scale[:, :width]
                keys = (normed * key_gain).astype(BF16)
                targets = (normed * value_gain * scale[:, width:]).astype(BF16)
                both = dot(keys, gate_up[...])
                back = dot(targets, down[...], NT)
                gate = both[:, :width]
                up = both[:, width:]
                sig = sigmoid(gate)
                act = gate * sig
                hidden = (act * up).astype(BF16)
                back_up = (back * act).astype(BF16)
                back_gate = (back * up * (sig + act * (1.0 - sig))).astype(BF16)
                backs = jnp.concatenate([back_gate, back_up], axis=1)
                return dot(keys, backs, TN), dot(hidden, targets, TN)

            return query, learn

        def answer(k):
            for i in range(tiles_row):
                read(k * tiles_row + i)[0]()

        def await_rows(k):
            arrived(xin.at[lane(c * toks + k, rows)], x_recv.at[c, k])

        def send_rows(k):
            block = xout.at[lane(c * toks + k, rows)]

            @pl.when(layer < layers - 1)
            def _():
                remote(
                    block,
                    xin.at[lane(c * toks + k, rows)],
                    x_send.at[c, k],
                    x_recv.at[c, k],
                    g,
                    t + 1,
                ).start()

            @pl.when(layer == layers - 1)
            def _():
                deliver(block, out.at[:, lane(head, width)], x_send.at[c, k], out_recv, c, k)

        def send_squares():
            @pl.when(layer < layers - 1)
            def _():
                @pl.loop(0, heads)
                def _(h):
                    remote(
                        sent_squares.at[c],
                        squares.at[c, head],
                        sq_send.at[c],
                        sq_recv.at[c],
                        h // per,
                        lax.rem(h, per) * layers + layer + 1,
                    ).start()

        @pl.when(c == groups - 1)
        def _():
            @pl.loop(0, toks)
            def _(k):
                await_rows(k)
                answer(k)
                send_rows(k)

            send_squares()

        @pl.when(c < groups - 1)
        def _():
            grad_gu[...] = jnp.zeros_like(grad_gu)
            grad_d[...] = jnp.zeros_like(grad_d)

            @pl.loop(0, toks)
            def _(k):
                await_rows(k)
                found = [read(k * tiles_row + i)[1]() for i in range(tiles_row)]
                grad_gu[...] += sum(f[0] for f in found)
                grad_d[...] += sum(f[1] for f in found)

            grads = (grad_gu[:, :width], grad_gu[:, width:], grad_d[...])
            start = tuple(
                v * lax.rsqrt(jnp.sum(v * v, axis=(0, 1), keepdims=True) + EPSILON) for v in grads
            )

            def beside(k, values):
                answer(k)
                values = newton_schulz(values)
                send_rows(k)
                return values

            moves = lax.fori_loop(0, toks, beside, start)
            send_squares()
            for _ in range(NS_STEPS - toks):
                moves = newton_schulz(moves)
            step = step_row * flags[c]
            for which in range(3):
                entering = state[which]
                moved = entering + step * moves[which]
                before = jnp.sum(entering * entering, axis=0, keepdims=True) + EPSILON
                after = jnp.sum(moved * moved, axis=0, keepdims=True) + EPSILON
                state[which] = moved * (jnp.sqrt(before) * lax.rsqrt(after))

    arrived(out, out_recv)

    for to_t in range(toks):
        holds, lay, slot = param_of(to_t)

        @pl.when(holds)
        def _():
            sent(initial.at[lay, :, slot], w_send.at[to_t], g, to_t)
            sent(packed.at[lay, slot], p_send.at[to_t], g, to_t)

    @pl.loop(0, groups)
    def _(to_g):
        sent(rates.at[layer], rate_send.at[to_g], to_g, t)

        @pl.when(layer < layers - 1)
        def _():
            arrived(squares.at[to_g], sq_send.at[to_g])

        @pl.loop(0, toks)
        def _(k):
            block = xout.at[lane(to_g * toks + k, rows)]

            @pl.when(layer < layers - 1)
            def _():
                arrived(block, x_send.at[to_g, k])

            @pl.when(layer == layers - 1)
            def _():
                sent(block, x_send.at[to_g, k], to_g, k)

    @pl.loop(0, heads)
    def _(h):
        to_g, to_t = h // per, lax.rem(h, per) * layers
        sent(totals, s_send.at[h], to_g, to_t)
        sent(tokens.at[:, lane(h, width)], t_send.at[h], to_g, to_t)


def head_body(tokens, learning_rates, channel_gains, fast_init, step_size, update_table):
    groups, toks = lax.axis_size("group"), lax.axis_size("tok")
    layers, _, owned, width, _ = fast_init.shape
    rows, channels = tokens.shape
    heads = owned * toks
    group_tok = rows * toks
    rates = learning_rates.reshape(layers, 1, group_tok)
    gains = channel_gains.reshape(layers, 5, owned, width).transpose(0, 2, 1, 3)
    steps = jnp.broadcast_to(step_size[:, :, None, None], (layers, owned, 3, width))
    packed = jnp.concatenate([gains, steps], axis=2)
    layer = lax.rem(lax.axis_index("tok"), layers)
    flag_row = lax.dynamic_index_in_dim(update_table, layer, 0, keepdims=False).astype(F32)
    flags = jnp.broadcast_to(flag_row[:, None, None], (groups, 1, width))
    tile = 512
    sizes = (groups, toks, layers, heads, owned, rows, width, tile)
    vmem = pl.BlockSpec(memory_space=pltpu.VMEM)
    anywhere = pl.BlockSpec(memory_space=pl.ANY)
    dma = pltpu.SemaphoreType.DMA
    return pl.pallas_call(
        functools.partial(chain_kernel, sizes),
        out_shape=jax.ShapeDtypeStruct((rows, channels), BF16),
        in_specs=[vmem, vmem, vmem, vmem, anywhere],
        out_specs=anywhere,
        scratch_shapes=[
            pltpu.VMEM((groups * group_tok, width), BF16),
            pltpu.VMEM((groups * group_tok, width), BF16),
            pltpu.VMEM((groups, heads, 1, group_tok), F32),
            pltpu.VMEM((groups, 1, group_tok), F32),
            pltpu.VMEM((groups, 1, group_tok), F32),
            pltpu.VMEM((8, width), F32),
            pltpu.VMEM((3, width, width), F32),
            pltpu.VMEM((1, rows), F32),
            pltpu.VMEM((16, group_tok), BF16),
            pltpu.VMEM((width, 2 * width), BF16),
            pltpu.VMEM((width, width), BF16),
            pltpu.VMEM((width, 2 * width), F32),
            pltpu.VMEM((width, width), F32),
            dma((groups, toks)),
            dma((groups, toks)),
            dma((groups,)),
            dma((groups,)),
            dma,
            dma((groups,)),
            dma,
            dma((toks,)),
            dma,
            dma((toks,)),
            dma((heads,)),
            dma((heads,)),
            dma,
        ],
        compiler_params=pltpu.CompilerParams(
            collective_id=0, has_side_effects=True, vmem_limit_bytes=48 * 1024 * 1024
        ),
    )(tokens, rates, packed, flags, fast_init)


def plan(mesh, tokens, fast_init):
    groups, toks = mesh.shape["group"], mesh.shape["tok"]
    layers, _, heads, width, _ = fast_init.shape
    rows = tokens.shape[0] // (groups * toks)
    fits = groups * toks == layers * heads and toks % layers == 0 and heads % toks == 0
    fits = fits and toks <= NS_STEPS and rows % 512 == 0 and width % 128 == 0
    return head_body if fits and tokens.shape[0] * width <= 4 * 1024 * 1024 else body


def solution(mesh):
    in_specs = (
        P(("group", "tok"), None),
        P(None, "group"),
        P(None, None, "tok"),
        P(None, None, "tok", None, None),
        P(None, "tok"),
        P(),
    )
    out_specs = P(("group", "tok"), None)
    def run(*args):
        chosen = plan(mesh, args[0], args[3])
        return jax.shard_map(
            chosen, mesh=mesh, in_specs=in_specs, out_specs=out_specs, check_vma=False
        )(*args)

    return run
```
